32 devices in a mesh: batch: 16 (over z, y, core), rep: 2 (over x).
Axes of the slice: x: 2, y: 2, z: 4, core: 2. Of those that a mesh axis runs over, the one named last changes fastest.
Arguments:
- image_embed: bfloat16 [2048, 1024], P('batch'), may hold values from -2 to 2
- text_embed: bfloat16 [2048, 1024], P(('batch', 'rep')), may hold values from -2 to 2
- logit_scale: float32 [1], replicated, may hold values from 50 to 100
Outputs:
- mean_loss: float32 [], replicated
- image_grad: float32 [2048, 1024], P(('batch', 'rep'))
- text_grad: float32 [2048, 1024], P(('batch', 'rep'))
The draws below stay inside these ranges and needn't reach their ends.
All inputs are finite; a program needn't handle non-finite values.
Results may differ from the reference program's by a relative error of at most 0.0025.
Values may be sent and summed in bfloat16 or wider, within the bound.
A program may use at most 128 MiB of HBM per device.

```python
import math
import jax
import jax.numpy as jnp
from jax import lax

D = 1024
PAIRS = 2048


def pair_draw(key):
    base_key = jax.random.fold_in(key, 17)
    keys = jax.random.split(base_key, 2)
    text_rows = jax.random.normal(keys[0], (PAIRS, D), jnp.float32) * D ** (-0.5)
    image_rows = jax.random.normal(keys[1], (PAIRS, D), jnp.float32) * D ** (-0.5)
    return (jnp.clip(image_rows, -2.0, 2.0), jnp.clip(text_rows, -2.0, 2.0))


def draw_image_embed(key, part):
    return pair_draw(key)[0].astype(jnp.bfloat16)


def draw_text_embed(key, part):
    return pair_draw(key)[1].astype(jnp.bfloat16)


def setup_inputs(seed: int = 0) -> dict:
    seeds = jax.random.split(jax.random.key(seed), 4)
    image_embed = draw_image_embed(jax.random.fold_in(seeds[3], 71), 0)
    text_embed = draw_text_embed(jax.random.fold_in(seeds[3], 71), 0)
    logit_scale = jnp.clip(jnp.exp(jax.random.uniform(seeds[2], (1,), jnp.float32, math.log(50.0), math.log(100.0))), 50.0, 100.0)
    return {"image_embed": image_embed, "text_embed": text_embed, "logit_scale": logit_scale}


def scores_of(left_rows, right_rows, scale_value):
    return scale_value * lax.dot_general(left_rows, right_rows, (((1,), (1,)), ((), ())), preferred_element_type=jnp.float32)


def reference(image_embed, text_embed, logit_scale):
    scale_value = logit_scale[0]
    block_rows = math.gcd(PAIRS, 1024)
    block_count = PAIRS // block_rows
    starts = (jnp.arange(block_count) * block_rows).astype(jnp.int32)

    def lse_rows(first_row, mine, other):
        picked = lax.dynamic_slice_in_dim(mine, first_row, block_rows, 0)
        scores = scores_of(picked, other, scale_value)
        biggest = jnp.max(scores, axis=1)
        return biggest + jnp.log(jnp.sum(jnp.exp(scores - biggest[:, None]), axis=1))

    row_lse = lax.map(lambda first_row: lse_rows(first_row, image_embed, text_embed), starts).reshape(PAIRS)
    col_lse = lax.map(lambda first_row: lse_rows(first_row, text_embed, image_embed), starts).reshape(PAIRS)
    diagonal = scale_value * jnp.sum(image_embed.astype(jnp.float32) * text_embed.astype(jnp.float32), axis=1)
    mean_loss = jnp.sum(row_lse + col_lse - 2.0 * diagonal) / (2 * PAIRS)

    def grad_rows(first_row, mine, other, mine_lse, other_lse):
        picked = lax.dynamic_slice_in_dim(mine, first_row, block_rows, 0)
        picked_lse = lax.dynamic_slice_in_dim(mine_lse, first_row, block_rows, 0)
        scores = scores_of(picked, other, scale_value)
        row_ids = first_row + lax.broadcasted_iota(jnp.int32, scores.shape, 0)
        column_ids = lax.broadcasted_iota(jnp.int32, scores.shape, 1)
        match = (row_ids == column_ids).astype(jnp.float32)
        weights = (jnp.exp(scores - picked_lse[:, None]) + jnp.exp(scores - other_lse[None, :]) - 2.0 * match).astype(jnp.bfloat16)
        return (scale_value * 0.5) * jnp.dot(weights, other, preferred_element_type=jnp.float32)

    image_grad = lax.map(lambda first_row: grad_rows(first_row, image_embed, text_embed, row_lse, col_lse), starts).reshape(PAIRS, D)
    text_grad = lax.map(lambda first_row: grad_rows(first_row, text_embed, image_embed, col_lse, row_lse), starts).reshape(PAIRS, D)
    return (mean_loss, image_grad, text_grad)
```

```python
import functools

import jax
import jax.numpy as jnp
from jax import lax
from jax.experimental import pallas as pl
from jax.experimental.pallas import tpu as pltpu
from jax.sharding import PartitionSpec as P

MESH = pl.DeviceIdType.MESH
F32 = jnp.float32
BF16 = jnp.bfloat16


def nt_dot(a, b):
    return lax.dot_general(a, b, (((1,), (1,)), ((), ())), preferred_element_type=F32)


def tn_dot(a, b):
    return lax.dot_general(a, b, (((0,), (0,)), ((), ())), preferred_element_type=F32)


def kernel(
    low_count,
    high_count,
    pair_count,
    scale_ref,
    image_hbm,
    text_hbm,
    loss_ref,
    image_grad_ref,
    text_grad_ref,
    images,
    texts,
    scores,
    weights,
    row_stats,
    column_stats,
    row_loss,
    column_loss,
    image_out,
    text_out,
    image_in,
    text_in,
    image_own,
    text_own,
    local_sems,
    image_send,
    image_recv,
    text_send,
    text_recv,
    row_send,
    row_recv,
    column_send,
    column_recv,
    row_loss_send,
    row_loss_recv,
    column_loss_send,
    column_loss_recv,
    image_out_send,
    image_out_recv,
    text_out_send,
    text_out_recv,
):
    rows = images.shape[1]
    half = rows // 2
    columns = texts.shape[0]
    batch = lax.axis_index("batch")
    rep = lax.axis_index("rep")
    high = batch // low_count
    low = lax.rem(batch, low_count)
    member = low * 2 + rep
    member_count = 2 * low_count
    scale = scale_ref[0]

    def row_device(index):
        return (high * low_count + index // 2, jnp.int32(index % 2))

    def column_device(index):
        return (index * low_count + low, rep)

    own_text = pl.ds(pl.multiple_of(high * half, half), half)
    image_load = pltpu.make_async_copy(image_hbm, images.at[low], local_sems.at[0])
    text_load = pltpu.make_async_copy(text_hbm, texts.at[own_text], local_sems.at[1])
    image_load.start()
    text_load.start()

    barrier = pltpu.get_barrier_semaphore()
    for index in range(member_count):

        @pl.when(index != member)
        def _():
            pl.semaphore_signal(barrier, inc=1, device_id=row_device(index), device_id_type=MESH)

    for index in range(high_count):

        @pl.when(index != high)
        def _():
            pl.semaphore_signal(barrier, inc=1, device_id=column_device(index), device_id_type=MESH)

    pl.semaphore_wait(barrier, member_count + high_count - 2)

    def remote(source, target, send, recv, device):
        return pltpu.make_async_remote_copy(
            src_ref=source,
            dst_ref=target,
            send_sem=send,
            recv_sem=recv,
            device_id=device,
            device_id_type=MESH,
        )

    def text_slot(index):
        return texts.at[pl.ds(index * half, half)]

    def image_copy(index):
        return remote(
            images.at[low], images.at[low], image_send.at[index], image_recv.at[low],
            (high * low_count + index, rep),
        )

    def text_copy(index):
        return remote(
            texts.at[own_text], texts.at[own_text], text_send.at[index], text_recv.at[high],
            column_device(index),
        )

    def slot_copy(buffer, slot, send, recv, index, device):
        return remote(buffer.at[slot], buffer.at[slot], send.at[index], recv.at[slot], device)

    def row_copy(index):
        return slot_copy(row_stats, member, row_send, row_recv, index, row_device(index))

    def column_copy(index):
        return slot_copy(column_stats, high, column_send, column_recv, index, column_device(index))

    def row_loss_copy(index):
        return slot_copy(row_loss, high, row_loss_send, row_loss_recv, index, column_device(index))

    def column_loss_copy(index):
        return slot_copy(
            column_loss, member, column_loss_send, column_loss_recv, index, row_device(index)
        )

    def image_out_copy(index):
        return remote(
            image_out.at[index], image_in.at[member], image_out_send.at[index],
            image_out_recv.at[member], row_device(index),
        )

    def text_out_copy(index):
        return remote(
            text_out.at[index], text_in.at[high], text_out_send.at[index],
            text_out_recv.at[high], column_device(index),
        )

    def arrived(buffer, recv, index):
        remote(buffer, buffer, recv.at[index], recv.at[index], (batch, rep)).wait_recv()

    def each(count, own, action):
        for index in range(count):

            @pl.when(index != own)
            def _():
                action(index)

    text_load.wait()
    each(high_count, high, lambda index: text_copy(index).start())
    image_load.wait()
    each(low_count, low, lambda index: image_copy(index).start())

    each(high_count, high, lambda index: arrived(text_slot(index), text_recv, index))

    diag_start = rep * half
    row_iota = lax.broadcasted_iota(jnp.int32, (rows, columns), 0)
    column_iota = lax.broadcasted_iota(jnp.int32, (rows, columns), 1) - high * half
    in_diag = (column_iota >= 0) & (column_iota < half)

    def diag_of(index):
        return in_diag & (row_iota - diag_start == column_iota) & (low == index)

    lanes = lax.broadcasted_iota(jnp.int32, (rows, 128), 1)
    column_max = None
    diag_sum = jnp.zeros((1, columns), F32)
    for index in range(low_count):

        @pl.when(index != low)
        def _():
            arrived(images.at[index], image_recv, index)

        block = scale * nt_dot(images[index], texts[...])
        scores[index] = block
        row_max = jnp.max(block, axis=1, keepdims=True)
        row_sum = jnp.sum(jnp.exp(block - row_max), axis=1, keepdims=True)
        packed = jnp.where(lanes == 0, row_max, row_sum).T
        row_stats[member, 0:2, index * rows : (index + 1) * rows] = packed[0:2]
        block_max = jnp.max(block, axis=0, keepdims=True)
        new_max = block_max if column_max is None else jnp.maximum(column_max, block_max)
        block_sum = jnp.sum(jnp.exp(block - new_max), axis=0, keepdims=True)
        if column_max is None:
            column_sum = block_sum
        else:
            column_sum = column_sum * jnp.exp(column_max - new_max) + block_sum
        column_max = new_max
        diag_sum = diag_sum + jnp.sum(
            jnp.where(diag_of(index), block, 0.0), axis=0, keepdims=True
        )
    row_stats[member, 2:3, :] = jnp.full((1, low_count * rows), jnp.sum(diag_sum), F32)
    column_stats[high, 0:1, :] = column_max
    column_stats[high, 1:2, :] = column_sum
    each(high_count, high, lambda index: column_copy(index).start())
    each(member_count, member, lambda index: row_copy(index).start())

    def merged(stats, count):
        top = stats[0, 0:1, :]
        for index in range(1, count):
            top = jnp.maximum(top, stats[index, 0:1, :])
        total = jnp.zeros_like(top)
        for index in range(count):
            total = total + stats[index, 1:2, :] * jnp.exp(stats[index, 0:1, :] - top)
        return top + jnp.log(total)

    each(member_count, member, lambda index: arrived(row_stats.at[index], row_recv, index))
    row_lse = merged(row_stats, member_count)
    each(high_count, high, lambda index: arrived(column_stats.at[index], column_recv, index))
    column_lse = merged(column_stats, high_count)

    diag_total = row_stats[0, 2:3, 0:128]
    for index in range(1, member_count):
        diag_total = diag_total + row_stats[index, 2:3, 0:128]
    row_loss[high] = jnp.full((1, 128), jnp.sum(row_lse), F32) - 2.0 * diag_total
    column_loss[member] = jnp.full((1, 128), jnp.sum(column_lse), F32)
    each(high_count, high, lambda index: row_loss_copy(index).start())
    each(member_count, member, lambda index: column_loss_copy(index).start())

    for index in range(low_count):
        span = pl.ds(index * rows, rows)
        block = scores[index]
        spread = jnp.broadcast_to(row_lse[:, index * rows : (index + 1) * rows], (128, rows)).T
        weights[span] = (
            jnp.exp(block - spread[:, 0:1])
            + jnp.exp(block - column_lse)
            - jnp.where(diag_of(index), 2.0, 0.0)
        ).astype(BF16)

    per_dot = 128 // half
    for start in range(0, high_count, per_dot):
        part = tn_dot(
            weights[:, start * half : (start + per_dot) * half],
            images[...].reshape(low_count * rows, images.shape[2]),
        )
        for offset in range(per_dot):
            index = start + offset
            piece = part[offset * half : (offset + 1) * half]
            text_out[index] = piece.astype(BF16)

            @pl.when(index != high)
            def _():
                text_out_copy(index).start()

            @pl.when(index == high)
            def _():
                text_own[...] = piece

    for low_index in range(low_count):
        part = jnp.dot(
            weights[pl.ds(low_index * rows, rows)], texts[...], preferred_element_type=F32
        )
        for offset in range(2):
            index = 2 * low_index + offset
            piece = part[offset * half : (offset + 1) * half]
            image_out[index] = piece.astype(BF16)

            @pl.when(index != member)
            def _():
                image_out_copy(index).start()

            @pl.when(index == member)
            def _():
                image_own[...] = piece

    each(high_count, high, lambda index: arrived(row_loss.at[index], row_loss_recv, index))
    each(
        member_count, member, lambda index: arrived(column_loss.at[index], column_loss_recv, index)
    )
    total = row_loss[0]
    for index in range(1, high_count):
        total = total + row_loss[index]
    for index in range(member_count):
        total = total + column_loss[index]
    loss_ref[0, 0] = jnp.max(total) / (2 * pair_count)

    factor = scale * 0.5
    each(high_count, high, lambda index: arrived(text_in.at[index], text_out_recv, index))
    total = text_own[...]
    for index in range(1, high_count):
        total = total + text_in[lax.rem(high + index, high_count)].astype(F32)
    text_grad_ref[...] = factor * total
    each(member_count, member, lambda index: arrived(image_in.at[index], image_out_recv, index))
    total = image_own[...]
    for index in range(1, member_count):
        total = total + image_in[lax.rem(member + index, member_count)].astype(F32)
    image_grad_ref[...] = factor * total

    for count, own, copy in (
        (low_count, low, image_copy),
        (high_count, high, text_copy),
        (member_count, member, row_copy),
        (high_count, high, column_copy),
        (high_count, high, row_loss_copy),
        (member_count, member, column_loss_copy),
        (member_count, member, image_out_copy),
        (high_count, high, text_out_copy),
    ):
        each(count, own, lambda index: copy(index).wait_send())


def body(image_embed, text_embed, logit_scale):
    rows, width = image_embed.shape
    half = text_embed.shape[0]
    batch_count = lax.axis_size("batch")
    low_count = 1
    while (2 * low_count) ** 2 <= batch_count:
        low_count *= 2
    high_count = batch_count // low_count
    members = 2 * low_count
    columns = high_count * half
    vmem = pl.BlockSpec(memory_space=pltpu.VMEM)
    smem = pl.BlockSpec(memory_space=pltpu.SMEM)
    hbm = pl.BlockSpec(memory_space=pl.ANY)
    dma = pltpu.SemaphoreType.DMA

    def pair(count):
        return [dma((count,)), dma((count,))]

    loss, image_grad, text_grad = pl.pallas_call(
        functools.partial(kernel, low_count, high_count, rows * batch_count),
        out_shape=(
            jax.ShapeDtypeStruct((1, 1), F32),
            jax.ShapeDtypeStruct((half, width), F32),
            jax.ShapeDtypeStruct((half, width), F32),
        ),
        in_specs=[smem, hbm, hbm],
        out_specs=(smem, vmem, vmem),
        scratch_shapes=[
            pltpu.VMEM((low_count, rows, width), BF16),
            pltpu.VMEM((columns, width), BF16),
            pltpu.VMEM((low_count, rows, columns), F32),
            pltpu.VMEM((low_count * rows, columns), BF16),
            pltpu.VMEM((members, 4, low_count * rows), F32),
            pltpu.VMEM((high_count, 4, columns), F32),
            pltpu.VMEM((high_count, 1, 128), F32),
            pltpu.VMEM((members, 1, 128), F32),
            pltpu.VMEM((members, half, width), BF16),
            pltpu.VMEM((high_count, half, width), BF16),
            pltpu.VMEM((members, half, width), BF16),
            pltpu.VMEM((high_count, half, width), BF16),
            pltpu.VMEM((half, width), F32),
            pltpu.VMEM((half, width), F32),
            dma((2,)),
        ]
        + pair(low_count)
        + pair(high_count)
        + pair(members)
        + pair(high_count)
        + pair(high_count)
        + pair(members)
        + pair(members)
        + pair(high_count),
        compiler_params=pltpu.CompilerParams(
            collective_id=0, has_side_effects=True, vmem_limit_bytes=60 * 1024 * 1024
        ),
    )(logit_scale, image_embed, text_embed)
    return (loss.reshape(()), image_grad, text_grad)


def solution(mesh):
    in_specs = (P("batch", None), P(("batch", "rep"), None), P())
    out_specs = (P(), P(("batch", "rep"), None), P(("batch", "rep"), None))
    return jax.shard_map(body, mesh=mesh, in_specs=in_specs, out_specs=out_specs, check_vma=False)
```

```python
import functools

import jax
import jax.numpy as jnp
from jax import lax
from jax.experimental import pallas as pl
from jax.experimental.pallas import tpu as pltpu
from jax.sharding import PartitionSpec as P

MESH = pl.DeviceIdType.MESH
F32 = jnp.float32
BF16 = jnp.bfloat16


def nt_dot(a, b):
    return lax.dot_general(a, b, (((1,), (1,)), ((), ())), preferred_element_type=F32)


def tn_dot(a, b):
    return lax.dot_general(a, b, (((0,), (0,)), ((), ())), preferred_element_type=F32)


def kernel(
    low_count,
    high_count,
    pair_count,
    scale_ref,
    image_hbm,
    text_hbm,
    loss_ref,
    image_grad_ref,
    text_grad_ref,
    images,
    texts,
    scores,
    weights,
    row_stats,
    column_stats,
    row_loss,
    column_loss,
    image_out,
    text_out,
    image_in,
    text_in,
    image_own,
    text_own,
    text_held,
    text_relay,
    core_out,
    core_in,
    local_sems,
    image_send,
    image_recv,
    text_send,
    text_recv,
    row_send,
    row_recv,
    column_send,
    column_recv,
    row_loss_send,
    row_loss_recv,
    column_loss_send,
    column_loss_recv,
    image_out_send,
    image_out_recv,
    text_out_send,
    text_out_recv,
    core_send,
    core_recv,
    relay_recv,
):
    rows = images.shape[1]
    half = rows // 2
    columns = texts.shape[0]
    batch = lax.axis_index("batch")
    rep = lax.axis_index("rep")
    high = batch // low_count
    low = lax.rem(batch, low_count)
    member = low * 2 + rep
    member_count = 2 * low_count
    core = lax.rem(low, 2)
    place = low // 2 * 2 + rep
    scale = scale_ref[0]
    via = {3: (0, 1), 0: (3, 2)} if high_count == 4 else {}

    def row_device(index):
        return (high * low_count + index // 2, jnp.int32(index % 2))

    def column_device(index):
        return (index * low_count + low, rep)

    own_text = pl.ds(pl.multiple_of(high * half, half), half)
    image_load = pltpu.make_async_copy(image_hbm, images.at[low], local_sems.at[0])
    text_load = pltpu.make_async_copy(text_hbm, texts.at[own_text], local_sems.at[1])
    image_load.start()
    text_load.start()

    barrier = pltpu.get_barrier_semaphore()
    for index in range(member_count):

        @pl.when(index != member)
        def _():
            pl.semaphore_signal(barrier, inc=1, device_id=row_device(index), device_id_type=MESH)

    for index in range(high_count):

        @pl.when(index != high)
        def _():
            pl.semaphore_signal(barrier, inc=1, device_id=column_device(index), device_id_type=MESH)

    pl.semaphore_wait(barrier, member_count + high_count - 2)

    def remote(source, target, send, recv, device):
        return pltpu.make_async_remote_copy(
            src_ref=source,
            dst_ref=target,
            send_sem=send,
            recv_sem=recv,
            device_id=device,
            device_id_type=MESH,
        )

    def text_slot(index):
        return texts.at[pl.ds(index * half, half)]

    def image_copy(index):
        return remote(
            images.at[low], images.at[low], image_send.at[index], image_recv.at[low],
            (high * low_count + index, rep),
        )

    def text_copy(index):
        return remote(
            texts.at[own_text], texts.at[own_text], text_send.at[index], text_recv.at[high],
            column_device(index),
        )

    def slot_copy(buffer, slot, send, recv, index, device):
        return remote(buffer.at[slot], buffer.at[slot], send.at[index], recv.at[slot], device)

    def row_copy(index):
        return slot_copy(row_stats, member, row_send, row_recv, index, row_device(index))

    def column_copy(index):
        return slot_copy(column_stats, high, column_send, column_recv, index, column_device(index))

    def row_loss_copy(index):
        return slot_copy(row_loss, high, row_loss_send, row_loss_recv, index, column_device(index))

    def column_loss_copy(index):
        return slot_copy(
            column_loss, member, column_loss_send, column_loss_recv, index, row_device(index)
        )

    def image_out_copy(index):
        return remote(
            image_out.at[index], image_in.at[place], image_out_send.at[index],
            image_out_recv.at[place],
            (high * low_count + index // 2 * 2 + core, jnp.int32(index % 2)),
        )

    def core_copy(chip):
        pieces = pl.ds(2 * chip, 2)
        return remote(
            core_out.at[pieces], core_in.at[pieces], core_send.at[chip], core_recv.at[chip],
            (batch + 1 - 2 * core, rep),
        )

    def relay_copy(index, middle):
        return remote(
            text_out.at[index], text_relay, text_out_send.at[index], relay_recv.at[0],
            column_device(middle),
        )

    def text_out_copy(index):
        return remote(
            text_out.at[index], text_in.at[high], text_out_send.at[index],
            text_out_recv.at[high], column_device(index),
        )

    def arrived(buffer, recv, index):
        remote(buffer, buffer, recv.at[index], recv.at[index], (batch, rep)).wait_recv()

    def each(count, own, action):
        for index in range(count):

            @pl.when(index != own)
            def _():
                action(index)

    text_load.wait()
    each(high_count, high, lambda index: text_copy(index).start())
    image_load.wait()
    each(low_count, low, lambda index: image_copy(index).start())

    each(high_count, high, lambda index: arrived(text_slot(index), text_recv, index))

    diag_start = rep * half
    row_iota = lax.broadcasted_iota(jnp.int32, (rows, columns), 0)
    column_iota = lax.broadcasted_iota(jnp.int32, (rows, columns), 1) - high * half
    in_diag = (column_iota >= 0) & (column_iota < half)

    def diag_of(index):
        return in_diag & (row_iota - diag_start == column_iota) & (low == index)

    lanes = lax.broadcasted_iota(jnp.int32, (rows, 128), 1)
    span = low_count * rows
    column_max = None
    diag_sum = jnp.zeros((1, columns), F32)
    for index in range(low_count):

        @pl.when(index != low)
        def _():
            arrived(images.at[index], image_recv, index)

        block = scale * nt_dot(images[index], texts[...])
        scores[index] = block
        row_max = jnp.max(block, axis=1, keepdims=True)
        row_sum = jnp.sum(jnp.exp(block - row_max), axis=1, keepdims=True)
        packed = jnp.where(lanes == 0, row_max, row_sum).T
        here = index * rows
        row_stats[member, 0:1, here : here + rows] = packed[0:1]
        row_stats[member, 0:1, span + here : span + here + rows] = packed[1:2]
        block_max = jnp.max(block, axis=0, keepdims=True)
        new_max = block_max if column_max is None else jnp.maximum(column_max, block_max)
        block_sum = jnp.sum(jnp.exp(block - new_max), axis=0, keepdims=True)
        if column_max is None:
            column_sum = block_sum
        else:
            column_sum = column_sum * jnp.exp(column_max - new_max) + block_sum
        column_max = new_max
        diag_sum = diag_sum + jnp.sum(
            jnp.where(diag_of(index), block, 0.0), axis=0, keepdims=True
        )
    row_stats[member, 0:1, 2 * span :] = jnp.full((1, 128), jnp.sum(diag_sum), F32)
    column_stats[high, 0:1, 0:columns] = column_max
    column_stats[high, 0:1, columns:] = column_sum
    each(high_count, high, lambda index: column_copy(index).start())
    each(member_count, member, lambda index: row_copy(index).start())

    def merged(stats, count, size):
        top = stats[0, 0:1, 0:size]
        for index in range(1, count):
            top = jnp.maximum(top, stats[index, 0:1, 0:size])
        total = jnp.zeros_like(top)
        for index in range(count):
            total = total + stats[index, 0:1, size : 2 * size] * jnp.exp(
                stats[index, 0:1, 0:size] - top
            )
        return top + jnp.log(total)

    each(member_count, member, lambda index: arrived(row_stats.at[index], row_recv, index))
    row_lse = merged(row_stats, member_count, span)
    each(high_count, high, lambda index: arrived(column_stats.at[index], column_recv, index))
    column_lse = merged(column_stats, high_count, columns)

    diag_total = row_stats[0, 0:1, 2 * span :]
    for index in range(1, member_count):
        diag_total = diag_total + row_stats[index, 0:1, 2 * span :]
    row_loss[high] = jnp.full((1, 128), jnp.sum(row_lse), F32) - 2.0 * diag_total
    column_loss[member] = jnp.full((1, 128), jnp.sum(column_lse), F32)
    each(high_count, high, lambda index: row_loss_copy(index).start())
    each(member_count, member, lambda index: column_loss_copy(index).start())

    for index in range(low_count):
        block = scores[index]
        spread = jnp.broadcast_to(row_lse[:, index * rows : (index + 1) * rows], (128, rows)).T
        weights[pl.ds(index * rows, rows)] = (
            jnp.exp(block - spread[:, 0:1])
            + jnp.exp(block - column_lse)
            - jnp.where(diag_of(index), 2.0, 0.0)
        ).astype(BF16)

    def image_part(low_index):
        first = pl.multiple_of(low_index * rows, rows)
        return jnp.dot(weights[pl.ds(first, rows)], texts[...], preferred_element_type=F32)

    for chip in range(low_count // 2):
        part = image_part(2 * chip + 1 - core)
        core_out[2 * chip] = part[:half].astype(BF16)
        core_out[2 * chip + 1] = part[half:].astype(BF16)
        core_copy(chip).start()

    per_dot = 128 // half
    for start in range(0, high_count, per_dot):
        part = tn_dot(
            weights[:, start * half : (start + per_dot) * half],
            images[...].reshape(low_count * rows, images.shape[2]),
        )
        for offset in range(per_dot):
            index = start + offset
            piece = part[offset * half : (offset + 1) * half]
            text_out[index] = piece.astype(BF16)

            @pl.when(index == high)
            def _():
                text_own[...] = piece

            if index in via:

                @pl.when(high == via[index][1])
                def _():
                    text_held[...] = piece

    for index, (origin, middle) in via.items():

        @pl.when(high == origin)
        def _():
            relay_copy(index, middle).start()

    def direct(index):
        if index not in via:
            text_out_copy(index).start()
            return

        @pl.when((high != via[index][0]) & (high != via[index][1]))
        def _():
            text_out_copy(index).start()

    each(high_count, high, direct)

    for chip in range(low_count // 2):
        part = image_part(2 * chip + core)
        arrived(core_in.at[pl.ds(2 * chip, 2)], core_recv, chip)
        for offset in range(2):
            index = 2 * chip + offset
            piece = part[offset * half : (offset + 1) * half] + core_in[index].astype(F32)
            image_out[index] = piece.astype(BF16)

            @pl.when(index != place)
            def _():
                image_out_copy(index).start()

            @pl.when(index == place)
            def _():
                image_own[...] = piece

    for index, (origin, middle) in via.items():

        @pl.when(high == middle)
        def _():
            arrived(text_relay, relay_recv, 0)
            text_out[index] = (text_held[...] + text_relay[...].astype(F32)).astype(BF16)
            text_out_copy(index).start()

    each(high_count, high, lambda index: arrived(row_loss.at[index], row_loss_recv, index))
    each(
        member_count, member, lambda index: arrived(column_loss.at[index], column_loss_recv, index)
    )
    total = row_loss[0]
    for index in range(1, high_count):
        total = total + row_loss[index]
    for index in range(member_count):
        total = total + column_loss[index]
    loss_ref[0, 0] = jnp.max(total) / (2 * pair_count)

    def text_add(index):
        arrived(text_in.at[index], text_out_recv, index)
        text_own[...] += text_in[index].astype(F32)

    def text_join(index):
        senders = [entry[0] for target, entry in via.items() if high_count - 1 - index == target]
        if not senders or senders[0] != index:
            text_add(index)
            return

        @pl.when(high != high_count - 1 - index)
        def _():
            text_add(index)

    each(low_count, place, lambda index: arrived(image_in.at[index], image_out_recv, index))
    total = image_own[...]
    for index in range(1, low_count):
        total = total + image_in[lax.rem(place + index, low_count)].astype(F32)
    image_grad_ref[...] = total
    each(high_count, high, text_join)
    text_grad_ref[...] = text_own[...]

    for count, own, copy in (
        (low_count, low, image_copy),
        (high_count, high, text_copy),
        (member_count, member, row_copy),
        (high_count, high, column_copy),
        (high_count, high, row_loss_copy),
        (member_count, member, column_loss_copy),
        (low_count, place, image_out_copy),
        (high_count, high, text_out_copy),
    ):
        each(count, own, lambda index: copy(index).wait_send())
    for chip in range(low_count // 2):
        core_copy(chip).wait_send()


def body(image_embed, text_embed, logit_scale):
    rows, width = image_embed.shape
    half = text_embed.shape[0]
    batch_count = lax.axis_size("batch")
    low_count = 1
    while (2 * low_count) ** 2 <= batch_count:
        low_count *= 2
    high_count = batch_count // low_count
    members = 2 * low_count
    columns = high_count * half
    vmem = pl.BlockSpec(memory_space=pltpu.VMEM)
    smem = pl.BlockSpec(memory_space=pltpu.SMEM)
    hbm = pl.BlockSpec(memory_space=pl.ANY)
    dma = pltpu.SemaphoreType.DMA

    def pair(count):
        return [dma((count,)), dma((count,))]

    loss, image_grad, text_grad = pl.pallas_call(
        functools.partial(kernel, low_count, high_count, rows * batch_count),
        out_shape=(
            jax.ShapeDtypeStruct((1, 1), F32),
            jax.ShapeDtypeStruct((half, width), F32),
            jax.ShapeDtypeStruct((half, width), F32),
        ),
        in_specs=[smem, hbm, hbm],
        out_specs=(smem, vmem, vmem),
        scratch_shapes=[
            pltpu.VMEM((low_count, rows, width), BF16),
            pltpu.VMEM((columns, width), BF16),
            pltpu.VMEM((low_count, rows, columns), F32),
            pltpu.VMEM((low_count * rows, columns), BF16),
            pltpu.VMEM((members, 1, 2 * low_count * rows + 128), F32),
            pltpu.VMEM((high_count, 1, 2 * columns), F32),
            pltpu.VMEM((high_count, 1, 128), F32),
            pltpu.VMEM((members, 1, 128), F32),
            pltpu.VMEM((low_count, half, width), BF16),
            pltpu.VMEM((high_count, half, width), BF16),
            pltpu.VMEM((low_count, half, width), BF16),
            pltpu.VMEM((high_count, half, width), BF16),
            pltpu.VMEM((half, width), F32),
            pltpu.VMEM((half, width), F32),
            pltpu.VMEM((half, width), F32),
            pltpu.VMEM((half, width), BF16),
            pltpu.VMEM((low_count, half, width), BF16),
            pltpu.VMEM((low_count, half, width), BF16),
            dma((2,)),
        ]
        + pair(low_count)
        + pair(high_count)
        + pair(members)
        + pair(high_count)
        + pair(high_count)
        + pair(members)
        + pair(low_count)
        + pair(high_count)
        + pair(low_count // 2)
        + [dma((1,))],
        compiler_params=pltpu.CompilerParams(
            collective_id=0, has_side_effects=True, vmem_limit_bytes=60 * 1024 * 1024
        ),
    )(logit_scale, image_embed, text_embed)
    factor = logit_scale[0] * 0.5
    return (loss.reshape(()), factor * image_grad, factor * text_grad)


def solution(mesh):
    in_specs = (P("batch", None), P(("batch", "rep"), None), P())
    out_specs = (P(), P(("batch", "rep"), None), P(("batch", "rep"), None))
    return jax.shard_map(body, mesh=mesh, in_specs=in_specs, out_specs=out_specs, check_vma=False)
```

```python
import functools

import jax
import jax.numpy as jnp
from jax import lax
from jax.experimental import pallas as pl
from jax.experimental.pallas import tpu as pltpu
from jax.sharding import PartitionSpec as P

MESH = pl.DeviceIdType.MESH
F32 = jnp.float32
BF16 = jnp.bfloat16


def nt_dot(a, b):
    return lax.dot_general(a, b, (((1,), (1,)), ((), ())), preferred_element_type=F32)


def tn_dot(a, b):
    return lax.dot_general(a, b, (((0,), (0,)), ((), ())), preferred_element_type=F32)


def kernel(
    low_count,
    high_count,
    pair_count,
    scale_ref,
    image_hbm,
    text_hbm,
    loss_ref,
    image_grad_ref,
    text_grad_ref,
    images,
    texts,
    scores,
    weights,
    row_stats,
    column_stats,
    row_loss,
    column_loss,
    image_out,
    text_out,
    image_in,
    text_in,
    image_own,
    text_own,
    column_lses,
    core_out,
    core_in,
    local_sems,
    image_send,
    image_recv,
    text_send,
    text_recv,
    row_send,
    row_recv,
    column_send,
    column_recv,
    row_loss_send,
    row_loss_recv,
    column_loss_send,
    column_loss_recv,
    image_out_send,
    image_out_recv,
    text_out_send,
    text_out_recv,
    core_send,
    core_recv,
):
    rows = images.shape[1]
    half = rows // 2
    columns = texts.shape[0]
    batch = lax.axis_index("batch")
    rep = lax.axis_index("rep")
    high = batch // low_count
    low = lax.rem(batch, low_count)
    member = low * 2 + rep
    member_count = 2 * low_count
    core = lax.rem(low, 2)
    place = low // 2 * 2 + rep
    scale = scale_ref[0]

    group_width = 128
    per_group = group_width // half
    group_count = high_count // per_group
    own_group = high // per_group
    groups = [lax.rem(own_group + step, group_count) for step in range(group_count)]

    def row_device(index):
        return (high * low_count + index // 2, jnp.int32(index % 2))

    def column_device(index):
        return (index * low_count + low, rep)

    own_text = pl.ds(pl.multiple_of(high * half, half), half)
    image_load = pltpu.make_async_copy(image_hbm, images.at[low], local_sems.at[0])
    text_load = pltpu.make_async_copy(text_hbm, texts.at[own_text], local_sems.at[1])
    image_load.start()
    text_load.start()

    barrier = pltpu.get_barrier_semaphore()
    for index in range(member_count):

        @pl.when(index != member)
        def _():
            pl.semaphore_signal(barrier, inc=1, device_id=row_device(index), device_id_type=MESH)

    for index in range(high_count):

        @pl.when(index != high)
        def _():
            pl.semaphore_signal(barrier, inc=1, device_id=column_device(index), device_id_type=MESH)

    pl.semaphore_wait(barrier, member_count + high_count - 2)

    def remote(source, target, send, recv, device):
        return pltpu.make_async_remote_copy(
            src_ref=source,
            dst_ref=target,
            send_sem=send,
            recv_sem=recv,
            device_id=device,
            device_id_type=MESH,
        )

    def text_slot(index):
        return texts.at[pl.ds(pl.multiple_of(index * half, half), half)]

    def image_copy(chip):
        return remote(
            images.at[low], images.at[low], image_send.at[2 * chip + core], image_recv.at[low],
            (high * low_count + 2 * chip + core, rep),
        )

    def image_forward(chip):
        slot = 2 * chip + core
        return remote(
            images.at[slot], images.at[slot], image_send.at[2 * chip + 1 - core],
            image_recv.at[slot], (batch + 1 - 2 * core, rep),
        )

    def text_copy(index):
        return remote(
            texts.at[own_text], texts.at[own_text], text_send.at[index], text_recv.at[high],
            column_device(index),
        )

    def slot_copy(buffer, slot, send, recv, index, device):
        return remote(buffer.at[slot], buffer.at[slot], send.at[index], recv.at[slot], device)

    def row_copy(index):
        return slot_copy(row_stats, member, row_send, row_recv, index, row_device(index))

    def column_copy(index):
        return slot_copy(column_stats, high, column_send, column_recv, index, column_device(index))

    def row_loss_copy(index):
        return slot_copy(row_loss, high, row_loss_send, row_loss_recv, index, column_device(index))

    def column_loss_copy(index):
        return slot_copy(
            column_loss, member, column_loss_send, column_loss_recv, index, row_device(index)
        )

    def image_out_copy(index):
        return remote(
            image_out.at[index], image_in.at[place], image_out_send.at[index],
            image_out_recv.at[place],
            (high * low_count + index // 2 * 2 + core, jnp.int32(index % 2)),
        )

    def core_copy(chip):
        pieces = pl.ds(2 * chip, 2)
        return remote(
            core_out.at[pieces], core_in.at[pieces], core_send.at[chip], core_recv.at[chip],
            (batch + 1 - 2 * core, rep),
        )

    def text_out_copy(index):
        return remote(
            text_out.at[index], text_in.at[high], text_out_send.at[index],
            text_out_recv.at[high], column_device(index),
        )

    def arrived(buffer, recv, index):
        remote(buffer, buffer, recv.at[index], recv.at[index], (batch, rep)).wait_recv()

    def each(count, own, action):
        for index in range(count):

            @pl.when(index != own)
            def _():
                action(index)

    def group_members(step, action):
        for offset in range(per_group):
            index = groups[step] * per_group + offset

            @pl.when(index != high)
            def _():
                action(index)

    text_load.wait()
    for step in [*range(1, group_count), 0]:
        group_members(step, lambda index: text_copy(index).start())
    image_load.wait()
    chips = low_count // 2
    own_chip = low // 2
    each(chips, own_chip, lambda chip: image_copy(chip).start())
    image_forward(own_chip).start()

    def forward(chip):
        arrived(images.at[2 * chip + core], image_recv, 2 * chip + core)
        image_forward(chip).start()

    each(chips, own_chip, forward)
    for chip in range(chips):
        arrived(images.at[2 * chip + 1 - core], image_recv, 2 * chip + 1 - core)

    diag_start = rep * half
    row_iota = lax.broadcasted_iota(jnp.int32, (rows, group_width), 0)
    column_iota = lax.broadcasted_iota(jnp.int32, (rows, group_width), 1)
    column_iota = column_iota - lax.rem(high, per_group) * half
    in_diag = (column_iota >= 0) & (column_iota < half)

    def diag_of(index):
        return in_diag & (row_iota - diag_start == column_iota) & (low == index)

    def lanes_of(step, base=0):
        return pl.ds(pl.multiple_of(base + groups[step] * group_width, group_width), group_width)

    lanes = lax.broadcasted_iota(jnp.int32, (rows, 128), 1)
    span = low_count * rows
    row_max = [None] * low_count
    row_sum = [None] * low_count
    diag_sum = jnp.zeros((1, group_width), F32)
    for step in range(group_count):
        group_members(step, lambda index: arrived(text_slot(index), text_recv, index))
        blocks = []
        for index in range(low_count):
            block = scale * nt_dot(images[index], texts[lanes_of(step)])
            scores[groups[step], index] = block
            blocks.append(block)
            new_max = jnp.max(block, axis=1, keepdims=True)
            if step > 0:
                new_max = jnp.maximum(new_max, row_max[index])
            new_sum = jnp.sum(jnp.exp(block - new_max), axis=1, keepdims=True)
            if step > 0:
                new_sum = new_sum + row_sum[index] * jnp.exp(row_max[index] - new_max)
            row_max[index], row_sum[index] = new_max, new_sum
            if step == 0:
                diag_sum = diag_sum + jnp.sum(
                    jnp.where(diag_of(index), block, 0.0), axis=0, keepdims=True
                )
        tops = [jnp.max(block, axis=0, keepdims=True) for block in blocks]
        top = functools.reduce(jnp.maximum, tops)
        sums = [jnp.sum(jnp.exp(block - top), axis=0, keepdims=True) for block in blocks]
        column_stats[high, 0:1, lanes_of(step)] = top
        column_stats[high, 0:1, lanes_of(step, columns)] = sum(sums[1:], sums[0])
    for index in range(low_count):
        packed = jnp.where(lanes == 0, row_max[index], row_sum[index]).T
        here = index * rows
        row_stats[member, 0:1, here : here + rows] = packed[0:1]
        row_stats[member, 0:1, span + here : span + here + rows] = packed[1:2]
    row_stats[member, 0:1, 2 * span :] = jnp.full((1, 128), jnp.sum(diag_sum), F32)
    each(high_count, high, lambda index: column_copy(index).start())
    each(member_count, member, lambda index: row_copy(index).start())

    def merged(stats, count, size):
        top = stats[0, 0:1, 0:size]
        for index in range(1, count):
            top = jnp.maximum(top, stats[index, 0:1, 0:size])
        total = jnp.zeros_like(top)
        for index in range(count):
            total = total + stats[index, 0:1, size : 2 * size] * jnp.exp(
                stats[index, 0:1, 0:size] - top
            )
        return top + jnp.log(total)

    each(member_count, member, lambda index: arrived(row_stats.at[index], row_recv, index))
    row_lse = merged(row_stats, member_count, span)
    each(high_count, high, lambda index: arrived(column_stats.at[index], column_recv, index))
    column_lse = merged(column_stats, high_count, columns)

    diag_total = row_stats[0, 0:1, 2 * span :]
    for index in range(1, member_count):
        diag_total = diag_total + row_stats[index, 0:1, 2 * span :]
    row_loss[high] = jnp.full((1, 128), jnp.sum(row_lse), F32) - 2.0 * diag_total
    column_loss[member] = jnp.full((1, 128), jnp.sum(column_lse), F32)
    each(high_count, high, lambda index: row_loss_copy(index).start())
    each(member_count, member, lambda index: column_loss_copy(index).start())

    column_lses[...] = column_lse
    spread = [
        jnp.broadcast_to(row_lse[:, index * rows : (index + 1) * rows], (128, rows)).T
        for index in range(low_count)
    ]
    for step in [*range(1, group_count), 0]:
        here = lanes_of(step)
        for index in range(low_count):
            block = scores[groups[step], index]
            value = jnp.exp(block - spread[index][:, 0:1]) + jnp.exp(block - column_lses[:, here])
            if step == 0:
                value = value - jnp.where(diag_of(index), 2.0, 0.0)
            weights[pl.ds(index * rows, rows), here] = value.astype(BF16)
        part = tn_dot(weights[:, here], images[...].reshape(span, images.shape[2]))
        for offset in range(per_group):
            index = groups[step] * per_group + offset
            piece = part[offset * half : (offset + 1) * half]
            text_out[index] = piece.astype(BF16)

            @pl.when(index != high)
            def _():
                text_out_copy(index).start()

            if step == 0:

                @pl.when(index == high)
                def _():
                    text_own[...] = piece

    def image_part(low_index):
        first = pl.multiple_of(low_index * rows, rows)
        return jnp.dot(weights[pl.ds(first, rows)], texts[...], preferred_element_type=F32)

    for chip in range(low_count // 2):
        part = image_part(2 * chip + 1 - core)
        core_out[2 * chip] = part[:half].astype(BF16)
        core_out[2 * chip + 1] = part[half:].astype(BF16)
        core_copy(chip).start()

    for chip in range(low_count // 2):
        part = image_part(2 * chip + core)
        arrived(core_in.at[pl.ds(2 * chip, 2)], core_recv, chip)
        for offset in range(2):
            index = 2 * chip + offset
            piece = part[offset * half : (offset + 1) * half] + core_in[index].astype(F32)
            image_out[index] = piece.astype(BF16)

            @pl.when(index != place)
            def _():
                image_out_copy(index).start()

            @pl.when(index == place)
            def _():
                image_own[...] = piece

    each(high_count, high, lambda index: arrived(row_loss.at[index], row_loss_recv, index))
    each(
        member_count, member, lambda index: arrived(column_loss.at[index], column_loss_recv, index)
    )
    total = row_loss[0]
    for index in range(1, high_count):
        total = total + row_loss[index]
    for index in range(member_count):
        total = total + column_loss[index]
    loss_ref[0, 0] = jnp.max(total) / (2 * pair_count)

    def text_add(index):
        arrived(text_in.at[index], text_out_recv, index)
        text_own[...] += text_in[index].astype(F32)

    each(low_count, place, lambda index: arrived(image_in.at[index], image_out_recv, index))
    total = image_own[...]
    for index in range(1, low_count):
        total = total + image_in[lax.rem(place + index, low_count)].astype(F32)
    image_grad_ref[...] = total
    each(high_count, high, text_add)
    text_grad_ref[...] = text_own[...]

    for count, own, copy in (
        (chips, own_chip, image_copy),
        (high_count, high, text_copy),
        (member_count, member, row_copy),
        (high_count, high, column_copy),
        (high_count, high, row_loss_copy),
        (member_count, member, column_loss_copy),
        (low_count, place, image_out_copy),
        (high_count, high, text_out_copy),
    ):
        each(count, own, lambda index: copy(index).wait_send())
    for chip in range(low_count // 2):
        core_copy(chip).wait_send()
        image_forward(chip).wait_send()


def body(image_embed, text_embed, logit_scale):
    rows, width = image_embed.shape
    half = text_embed.shape[0]
    batch_count = lax.axis_size("batch")
    low_count = 1
    while (2 * low_count) ** 2 <= batch_count:
        low_count *= 2
    high_count = batch_count // low_count
    members = 2 * low_count
    columns = high_count * half
    vmem = pl.BlockSpec(memory_space=pltpu.VMEM)
    smem = pl.BlockSpec(memory_space=pltpu.SMEM)
    hbm = pl.BlockSpec(memory_space=pl.ANY)
    dma = pltpu.SemaphoreType.DMA

    def pair(count):
        return [dma((count,)), dma((count,))]

    loss, image_grad, text_grad = pl.pallas_call(
        functools.partial(kernel, low_count, high_count, rows * batch_count),
        out_shape=(
            jax.ShapeDtypeStruct((1, 1), F32),
            jax.ShapeDtypeStruct((half, width), F32),
            jax.ShapeDtypeStruct((half, width), F32),
        ),
        in_specs=[smem, hbm, hbm],
        out_specs=(smem, vmem, vmem),
        scratch_shapes=[
            pltpu.VMEM((low_count, rows, width), BF16),
            pltpu.VMEM((columns, width), BF16),
            pltpu.VMEM((columns // 128, low_count, rows, 128), F32),
            pltpu.VMEM((low_count * rows, columns), BF16),
            pltpu.VMEM((members, 1, 2 * low_count * rows + 128), F32),
            pltpu.VMEM((high_count, 1, 2 * columns), F32),
            pltpu.VMEM((high_count, 1, 128), F32),
            pltpu.VMEM((members, 1, 128), F32),
            pltpu.VMEM((low_count, half, width), BF16),
            pltpu.VMEM((high_count, half, width), BF16),
            pltpu.VMEM((low_count, half, width), BF16),
            pltpu.VMEM((high_count, half, width), BF16),
            pltpu.VMEM((half, width), F32),
            pltpu.VMEM((half, width), F32),
            pltpu.VMEM((1, columns), F32),
            pltpu.VMEM((low_count, half, width), BF16),
            pltpu.VMEM((low_count, half, width), BF16),
            dma((2,)),
        ]
        + pair(low_count)
        + pair(high_count)
        + pair(members)
        + pair(high_count)
        + pair(high_count)
        + pair(members)
        + pair(low_count)
        + pair(high_count)
        + pair(low_count // 2),
        compiler_params=pltpu.CompilerParams(
            collective_id=0, has_side_effects=True, vmem_limit_bytes=60 * 1024 * 1024
        ),
    )(logit_scale, image_embed, text_embed)
    factor = logit_scale[0] * 0.5
    return (loss.reshape(()), factor * image_grad, factor * text_grad)


def solution(mesh):
    in_specs = (P("batch", None), P(("batch", "rep"), None), P())
    out_specs = (P(), P(("batch", "rep"), None), P(("batch", "rep"), None))
    return jax.shard_map(body, mesh=mesh, in_specs=in_specs, out_specs=out_specs, check_vma=False)
```

```python
import functools

import jax
import jax.numpy as jnp
from jax import lax
from jax.experimental import pallas as pl
from jax.experimental.pallas import tpu as pltpu
from jax.sharding import PartitionSpec as P

MESH = pl.DeviceIdType.MESH
F32 = jnp.float32
BF16 = jnp.bfloat16


def nt_dot(a, b):
    return lax.dot_general(a, b, (((1,), (1,)), ((), ())), preferred_element_type=F32)


def tn_dot(a, b):
    return lax.dot_general(a, b, (((0,), (0,)), ((), ())), preferred_element_type=F32)


def kernel(
    low_count,
    high_count,
    pair_count,
    scale_ref,
    image_hbm,
    text_hbm,
    loss_ref,
    grads_ref,
    images,
    texts,
    scores,
    weights,
    row_stats,
    column_stats,
    row_loss,
    column_loss,
    image_out,
    text_out,
    image_in,
    text_in,
    image_own,
    text_own,
    column_lses,
    core_out,
    core_in,
    local_sems,
    image_send,
    image_recv,
    text_send,
    text_recv,
    row_send,
    row_recv,
    column_send,
    column_recv,
    row_loss_send,
    row_loss_recv,
    column_loss_send,
    column_loss_recv,
    image_out_send,
    image_out_recv,
    text_out_send,
    text_out_recv,
    core_send,
    core_recv,
):
    rows = images.shape[1]
    half = rows // 2
    columns = texts.shape[0]
    batch = lax.axis_index("batch")
    rep = lax.axis_index("rep")
    high = batch // low_count
    low = lax.rem(batch, low_count)
    member = low * 2 + rep
    member_count = 2 * low_count
    core = lax.rem(low, 2)
    place = low // 2 * 2 + rep
    scale = scale_ref[0]

    group_width = 128
    per_group = group_width // half
    group_count = high_count // per_group
    own_group = high // per_group
    groups = [lax.rem(own_group + step, group_count) for step in range(group_count)]

    def row_device(index):
        return (high * low_count + index // 2, jnp.int32(index % 2))

    def column_device(index):
        return (index * low_count + low, rep)

    own_text = pl.ds(pl.multiple_of(high * half, half), half)
    image_load = pltpu.make_async_copy(image_hbm, images.at[low], local_sems.at[0])
    text_load = pltpu.make_async_copy(text_hbm, texts.at[own_text], local_sems.at[1])
    image_load.start()
    text_load.start()

    barrier = pltpu.get_barrier_semaphore()
    for index in range(member_count):

        @pl.when(index != member)
        def _():
            pl.semaphore_signal(barrier, inc=1, device_id=row_device(index), device_id_type=MESH)

    for index in range(high_count):

        @pl.when(index != high)
        def _():
            pl.semaphore_signal(barrier, inc=1, device_id=column_device(index), device_id_type=MESH)

    pl.semaphore_wait(barrier, member_count + high_count - 2)

    def remote(source, target, send, recv, device):
        return pltpu.make_async_remote_copy(
            src_ref=source,
            dst_ref=target,
            send_sem=send,
            recv_sem=recv,
            device_id=device,
            device_id_type=MESH,
        )

    def text_slot(index):
        return texts.at[pl.ds(pl.multiple_of(index * half, half), half)]

    def image_copy(chip):
        return remote(
            images.at[low], images.at[low], image_send.at[2 * chip + core], image_recv.at[low],
            (high * low_count + 2 * chip + core, rep),
        )

    def image_forward(chip):
        slot = 2 * chip + core
        return remote(
            images.at[slot], images.at[slot], image_send.at[2 * chip + 1 - core],
            image_recv.at[slot], (batch + 1 - 2 * core, rep),
        )

    def text_copy(index):
        return remote(
            texts.at[own_text], texts.at[own_text], text_send.at[index], text_recv.at[high],
            column_device(index),
        )

    def slot_copy(buffer, slot, send, recv, index, device):
        return remote(buffer.at[slot], buffer.at[slot], send.at[index], recv.at[slot], device)

    def row_copy(index):
        return slot_copy(row_stats, member, row_send, row_recv, index, row_device(index))

    def column_copy(index):
        return slot_copy(column_stats, high, column_send, column_recv, index, column_device(index))

    def row_loss_copy(index):
        return slot_copy(row_loss, high, row_loss_send, row_loss_recv, index, column_device(index))

    def column_loss_copy(index):
        return slot_copy(
            column_loss, member, column_loss_send, column_loss_recv, index, row_device(index)
        )

    def image_out_copy(index):
        return remote(
            image_out.at[index], image_in.at[place], image_out_send.at[index],
            image_out_recv.at[place],
            (high * low_count + index // 2 * 2 + core, jnp.int32(index % 2)),
        )

    def core_copy(chip):
        pieces = pl.ds(2 * chip, 2)
        return remote(
            core_out.at[pieces], core_in.at[pieces], core_send.at[chip], core_recv.at[chip],
            (batch + 1 - 2 * core, rep),
        )

    def text_out_copy(index):
        return remote(
            text_out.at[index], text_in.at[high], text_out_send.at[index],
            text_out_recv.at[high], column_device(index),
        )

    def arrived(buffer, recv, index):
        remote(buffer, buffer, recv.at[index], recv.at[index], (batch, rep)).wait_recv()

    def each(count, own, action):
        for index in range(count):

            @pl.when(index != own)
            def _():
                action(index)

    def group_members(step, action):
        for offset in range(per_group):
            index = groups[step] * per_group + offset

            @pl.when(index != high)
            def _():
                action(index)

    text_load.wait()
    for step in [*range(1, group_count), 0]:
        group_members(step, lambda index: text_copy(index).start())
    image_load.wait()
    chips = low_count // 2
    own_chip = low // 2
    each(chips, own_chip, lambda chip: image_copy(chip).start())
    image_forward(own_chip).start()

    def forward(chip):
        arrived(images.at[2 * chip + core], image_recv, 2 * chip + core)
        image_forward(chip).start()

    each(chips, own_chip, forward)
    for chip in range(chips):
        arrived(images.at[2 * chip + 1 - core], image_recv, 2 * chip + 1 - core)

    diag_start = rep * half
    row_iota = lax.broadcasted_iota(jnp.int32, (rows, group_width), 0)
    column_iota = lax.broadcasted_iota(jnp.int32, (rows, group_width), 1)
    column_iota = column_iota - lax.rem(high, per_group) * half
    in_diag = (column_iota >= 0) & (column_iota < half)

    def diag_of(index):
        return in_diag & (row_iota - diag_start == column_iota) & (low == index)

    def lanes_of(step, base=0):
        return pl.ds(pl.multiple_of(base + groups[step] * group_width, group_width), group_width)

    lanes = lax.broadcasted_iota(jnp.int32, (rows, 128), 1)
    span = low_count * rows
    row_max = [None] * low_count
    row_sum = [None] * low_count
    diag_sum = jnp.zeros((1, group_width), F32)
    for step in range(group_count):
        group_members(step, lambda index: arrived(text_slot(index), text_recv, index))
        blocks = []
        for index in range(low_count):
            block = scale * nt_dot(images[index], texts[lanes_of(step)])
            scores[groups[step], index] = block
            blocks.append(block)
            new_max = jnp.max(block, axis=1, keepdims=True)
            if step > 0:
                new_max = jnp.maximum(new_max, row_max[index])
            new_sum = jnp.sum(jnp.exp(block - new_max), axis=1, keepdims=True)
            if step > 0:
                new_sum = new_sum + row_sum[index] * jnp.exp(row_max[index] - new_max)
            row_max[index], row_sum[index] = new_max, new_sum
            if step == 0:
                diag_sum = diag_sum + jnp.sum(
                    jnp.where(diag_of(index), block, 0.0), axis=0, keepdims=True
                )
        tops = [jnp.max(block, axis=0, keepdims=True) for block in blocks]
        top = functools.reduce(jnp.maximum, tops)
        sums = [jnp.sum(jnp.exp(block - top), axis=0, keepdims=True) for block in blocks]
        column_stats[high, 0:1, lanes_of(step)] = top
        column_stats[high, 0:1, lanes_of(step, columns)] = sum(sums[1:], sums[0])
    for index in range(low_count):
        packed = jnp.where(lanes == 0, row_max[index], row_sum[index]).T
        here = index * rows
        row_stats[member, 0:1, here : here + rows] = packed[0:1]
        row_stats[member, 0:1, span + here : span + here + rows] = packed[1:2]
    row_stats[member, 0:1, 2 * span :] = jnp.full((1, 128), jnp.sum(diag_sum), F32)
    each(high_count, high, lambda index: column_copy(index).start())
    each(member_count, member, lambda index: row_copy(index).start())

    def merged(stats, count, size):
        top = stats[0, 0:1, 0:size]
        for index in range(1, count):
            top = jnp.maximum(top, stats[index, 0:1, 0:size])
        total = jnp.zeros_like(top)
        for index in range(count):
            total = total + stats[index, 0:1, size : 2 * size] * jnp.exp(
                stats[index, 0:1, 0:size] - top
            )
        return top + jnp.log(total)

    each(member_count, member, lambda index: arrived(row_stats.at[index], row_recv, index))
    row_lse = merged(row_stats, member_count, span)
    each(high_count, high, lambda index: arrived(column_stats.at[index], column_recv, index))
    column_lse = merged(column_stats, high_count, columns)

    diag_total = row_stats[0, 0:1, 2 * span :]
    for index in range(1, member_count):
        diag_total = diag_total + row_stats[index, 0:1, 2 * span :]
    row_loss[high] = jnp.full((1, 128), jnp.sum(row_lse), F32) - 2.0 * diag_total
    column_loss[member] = jnp.full((1, 128), jnp.sum(column_lse), F32)
    each(high_count, high, lambda index: row_loss_copy(index).start())
    each(member_count, member, lambda index: column_loss_copy(index).start())

    column_lses[...] = column_lse
    spread = [
        jnp.broadcast_to(row_lse[:, index * rows : (index + 1) * rows], (128, rows)).T
        for index in range(low_count)
    ]
    def text_part(step):
        here = lanes_of(step)
        part = tn_dot(weights[:, here], images[...].reshape(span, images.shape[2]))
        for offset in range(per_group):
            index = groups[step] * per_group + offset
            piece = part[offset * half : (offset + 1) * half]
            text_out[index] = piece.astype(BF16)

            @pl.when(index != high)
            def _():
                text_out_copy(index).start()

            if step == 0:

                @pl.when(index == high)
                def _():
                    text_own[...] = piece

    for step in [*range(1, group_count), 0]:
        here = lanes_of(step)
        for index in range(low_count):
            block = scores[groups[step], index]
            value = jnp.exp(block - spread[index][:, 0:1]) + jnp.exp(block - column_lses[:, here])
            if step == 0:
                value = value - jnp.where(diag_of(index), 2.0, 0.0)
            weights[pl.ds(index * rows, rows), here] = value.astype(BF16)
        if step > 0:
            text_part(step)

    def image_part(low_index):
        first = pl.multiple_of(low_index * rows, rows)
        return jnp.dot(weights[pl.ds(first, rows)], texts[...], preferred_element_type=F32)

    for chip in range(low_count // 2):
        part = image_part(2 * chip + 1 - core)
        core_out[2 * chip] = part[:half].astype(BF16)
        core_out[2 * chip + 1] = part[half:].astype(BF16)
        core_copy(chip).start()

    text_part(0)

    for chip in range(low_count // 2):
        part = image_part(2 * chip + core)
        arrived(core_in.at[pl.ds(2 * chip, 2)], core_recv, chip)
        for offset in range(2):
            index = 2 * chip + offset
            piece = part[offset * half : (offset + 1) * half] + core_in[index].astype(F32)
            image_out[index] = piece.astype(BF16)

            @pl.when(index != place)
            def _():
                image_out_copy(index).start()

            @pl.when(index == place)
            def _():
                image_own[...] = piece

    each(high_count, high, lambda index: arrived(row_loss.at[index], row_loss_recv, index))
    each(
        member_count, member, lambda index: arrived(column_loss.at[index], column_loss_recv, index)
    )
    total = row_loss[0]
    for index in range(1, high_count):
        total = total + row_loss[index]
    for index in range(member_count):
        total = total + column_loss[index]
    loss_ref[0, 0] = jnp.max(total) / (2 * pair_count)

    def text_add(index):
        arrived(text_in.at[index], text_out_recv, index)
        text_own[...] += text_in[index].astype(F32)

    each(low_count, place, lambda index: arrived(image_in.at[index], image_out_recv, index))
    total = image_own[...]
    for index in range(1, low_count):
        total = total + image_in[lax.rem(place + index, low_count)].astype(F32)
    grads_ref[0] = total
    each(high_count, high, text_add)
    grads_ref[1] = text_own[...]

    for count, own, copy in (
        (chips, own_chip, image_copy),
        (high_count, high, text_copy),
        (member_count, member, row_copy),
        (high_count, high, column_copy),
        (high_count, high, row_loss_copy),
        (member_count, member, column_loss_copy),
        (low_count, place, image_out_copy),
        (high_count, high, text_out_copy),
    ):
        each(count, own, lambda index: copy(index).wait_send())
    for chip in range(low_count // 2):
        core_copy(chip).wait_send()
        image_forward(chip).wait_send()


def body(image_embed, text_embed, logit_scale):
    rows, width = image_embed.shape
    half = text_embed.shape[0]
    batch_count = lax.axis_size("batch")
    low_count = 1
    while (2 * low_count) ** 2 <= batch_count:
        low_count *= 2
    high_count = batch_count // low_count
    members = 2 * low_count
    columns = high_count * half
    vmem = pl.BlockSpec(memory_space=pltpu.VMEM)
    smem = pl.BlockSpec(memory_space=pltpu.SMEM)
    hbm = pl.BlockSpec(memory_space=pl.ANY)
    dma = pltpu.SemaphoreType.DMA

    def pair(count):
        return [dma((count,)), dma((count,))]

    loss, grads = pl.pallas_call(
        functools.partial(kernel, low_count, high_count, rows * batch_count),
        out_shape=(
            jax.ShapeDtypeStruct((1, 1), F32),
            jax.ShapeDtypeStruct((2, half, width), F32),
        ),
        in_specs=[smem, hbm, hbm],
        out_specs=(smem, vmem),
        scratch_shapes=[
            pltpu.VMEM((low_count, rows, width), BF16),
            pltpu.VMEM((columns, width), BF16),
            pltpu.VMEM((columns // 128, low_count, rows, 128), F32),
            pltpu.VMEM((low_count * rows, columns), BF16),
            pltpu.VMEM((members, 1, 2 * low_count * rows + 128), F32),
            pltpu.VMEM((high_count, 1, 2 * columns), F32),
            pltpu.VMEM((high_count, 1, 128), F32),
            pltpu.VMEM((members, 1, 128), F32),
            pltpu.VMEM((low_count, half, width), BF16),
            pltpu.VMEM((high_count, half, width), BF16),
            pltpu.VMEM((low_count, half, width), BF16),
            pltpu.VMEM((high_count, half, width), BF16),
            pltpu.VMEM((half, width), F32),
            pltpu.VMEM((half, width), F32),
            pltpu.VMEM((1, columns), F32),
            pltpu.VMEM((low_count, half, width), BF16),
            pltpu.VMEM((low_count, half, width), BF16),
            dma((2,)),
        ]
        + pair(low_count)
        + pair(high_count)
        + pair(members)
        + pair(high_count)
        + pair(high_count)
        + pair(members)
        + pair(low_count)
        + pair(high_count)
        + pair(low_count // 2),
        compiler_params=pltpu.CompilerParams(
            collective_id=0, has_side_effects=True, vmem_limit_bytes=60 * 1024 * 1024
        ),
    )(logit_scale, image_embed, text_embed)
    factor = logit_scale[0] * 0.5
    return (loss.reshape(()), factor * grads[0], factor * grads[1])


def solution(mesh):
    in_specs = (P("batch", None), P(("batch", "rep"), None), P())
    out_specs = (P(), P(("batch", "rep"), None), P(("batch", "rep"), None))
    return jax.shard_map(body, mesh=mesh, in_specs=in_specs, out_specs=out_specs, check_vma=False)
```
